32 devices in a mesh: state: 32 (over z, y, x, core).
Axes of the slice: x: 2, y: 2, z: 4, core: 2. Of those that a mesh axis runs over, the one named last changes fastest.
Arguments:
- transitions: float32 [4096, 16, 4096], P('state'), may hold values from 0 to 1, as said below
- costs: float32 [4096, 16, 128], P('state'), may hold values from 0 to 4
- valid_counts: int32 [4096], P('state'), may hold values from 1 to 16
- start_values: float32 [4096, 128], P('state'), may hold values from -12 to 12
- ref_state: int32 [1], replicated, may hold values from 0 to 4095
Outputs:
- relative_values: float32 [4096, 128], P('state')
- lower_bounds: float32 [4, 128], replicated
- upper_bounds: float32 [4, 128], replicated
The draws below stay inside these ranges and needn't reach their ends.
Inputs may be any that keep to these rules, and one draw needn't show every extreme that they name: Every entry is nonnegative and each row transitions[s, a, :] sums to one up to float32 rounding. Actions 0 to valid_counts[s] - 1 are allowed in state s.
All inputs are finite; a program needn't handle non-finite values.
Results may differ from the reference program's by a relative error of at most 0.00017.
Values sent between devices are 32-bit elements; how exact they have to be, the bound alone decides.
A program may use at most 64 MiB of HBM per device.

```python
import jax
import jax.numpy as jnp
from jax import lax

STATES = 4096
ACTIONS = 16
SCENARIOS = 128
ITERS = 4


def draw_transitions(key, part):
    sigma = 2.0
    raw = jnp.exp(sigma * jax.random.normal(key, (STATES, ACTIONS, STATES), jnp.float32))
    return raw / jnp.sum(raw, axis=2, keepdims=True)


def place_ends(values, stream_key, low, top_value):
    extent = values.shape
    index_at = [jax.random.randint(jax.random.fold_in(stream_key, axis), (), 0, extent[axis]) for axis in range(len(extent))]
    values = values.at[tuple(index_at)].set(low)
    longest = extent.index(max(extent))
    index_at[longest] = (index_at[longest] + 1) % extent[longest]
    return values.at[tuple(index_at)].set(top_value)


def level_of(stream_key, dims, cuts, low, largest):
    def one(position, blocks):
        steps = jax.random.uniform(jax.random.fold_in(jax.random.fold_in(stream_key, 6), position), (blocks,), jnp.float32, low / len(cuts), largest / len(cuts))
        return jnp.repeat(jnp.exp(steps), dims[position] // blocks).reshape((-1,) + (1,) * (len(dims) - position - 1))

    factor_of = one(*cuts[0])
    for cut in cuts[1:]:
        factor_of = factor_of * one(*cut)
    return factor_of


def normal_values(stream_key, dims, deviation, bound, shards=(), held_as=jnp.bfloat16):
    loudness = level_of(stream_key, dims, shards, -0.22, 0.18) if shards else 1.0
    values = jax.random.normal(stream_key, dims, jnp.float32) * deviation * loudness
    return jnp.minimum(jnp.maximum(values, -bound), bound).astype(held_as)


def setup_inputs(seed: int = 0) -> dict:
    streams_of = jax.random.split(jax.random.key(seed), 6)
    return {
        "transitions": draw_transitions(jax.random.fold_in(streams_of[5], 71), 0),
        "costs": jnp.clip(4.0 * jax.random.uniform(streams_of[1], (STATES, ACTIONS, SCENARIOS), jnp.float32) ** level_of(streams_of[1], (STATES, ACTIONS, SCENARIOS), ((0, 32),), -0.2, 0.2), 0.0, 4.0),
        "valid_counts": place_ends(jax.random.randint(streams_of[2], (STATES,), 1, ACTIONS + 1), jax.random.fold_in(streams_of[2], 1), 1, ACTIONS).astype(jnp.int32),
        "start_values": normal_values(streams_of[3], (STATES, SCENARIOS), 2.0, 12.0, ((0, 32),), jnp.float32),
        "ref_state": jax.random.randint(streams_of[4], (1,), 0, STATES).astype(jnp.int32),
    }


big_value = 1e30


def reference(transitions, costs, valid_counts, start_values, ref_state):
    flat_rows = transitions.reshape(STATES * ACTIONS, STATES)
    allowed = jnp.arange(ACTIONS, dtype=jnp.int32)[None, :] < valid_counts[:, None]
    relative = start_values
    lower_list = []
    upper_list = []
    for iteration in range(ITERS):
        expected = jnp.dot(flat_rows, relative, precision=lax.Precision.HIGHEST, preferred_element_type=jnp.float32)
        q_values = costs + expected.reshape(STATES, ACTIONS, SCENARIOS)
        q_values = jnp.where(allowed[:, :, None], q_values, jnp.float32(big_value))
        best_value = jnp.min(q_values, axis=1)
        increase = best_value - relative
        lower_list.append(jnp.min(increase, axis=0))
        upper_list.append(jnp.max(increase, axis=0))
        ref_row = lax.dynamic_slice_in_dim(best_value, ref_state[0].astype(jnp.int32), 1, 0)
        relative = best_value - ref_row
    return relative, jnp.stack(lower_list), jnp.stack(upper_list)
```

```python
import functools

import jax
import jax.numpy as jnp
from jax import lax
from jax.experimental import pallas as pl
from jax.experimental.pallas import tpu as pltpu
from jax.sharding import PartitionSpec as P

ITERS = 4
PLANE = 8
MESH = pl.DeviceIdType.MESH

big_value = 1e30


def kernel(
    n, vc_ref, ref_ref, p_hbm, cost_hbm, start_hbm,
    rel_ref, low_ref, up_ref,
    field, pmat, wmat, acc, costs, stage, sbuf, rbuf,
    stage_sem, in_sem, send_sem, recv_sem, rsend_sem, rrecv_sem,
):
    planes = n // PLANE
    local, scen = start_hbm.shape
    rows, states = p_hbm.shape
    actions = rows // local
    kp = states // planes
    slots, chunk = stage.shape[0], stage.shape[1]
    chunks = rows // chunk
    me = lax.axis_index("state")
    z, low, core = me // PLANE, me % PLANE, me % 2
    dp = 1 - 2 * core
    dx = 2 - 4 * ((me // 2) % 2)
    dy = 4 - 8 * ((me // 4) % 2)
    da = dx + core * (dy - dx)
    db = dy + core * (dx - dy)

    def load(c):
        slot = lax.rem(c, slots)
        return pltpu.make_async_copy(
            p_hbm.at[pl.ds(c * chunk, chunk)], stage.at[slot], stage_sem.at[slot]
        )

    start_copy = pltpu.make_async_copy(start_hbm, field.at[0, me], in_sem.at[0])
    cost_copy = pltpu.make_async_copy(cost_hbm, costs, in_sem.at[1])
    start_copy.start()
    for c in range(slots):
        load(c).start()
    cost_copy.start()

    barrier = pltpu.get_barrier_semaphore()
    for delta in (dp, da, db):
        pl.semaphore_signal(barrier, inc=1, device_id=(me + delta,), device_id_type=MESH)

    def greet(d, carry):
        pl.semaphore_signal(
            barrier, inc=1, device_id=(lax.rem(z + d, planes) * PLANE + low,), device_id_type=MESH
        )
        return carry

    lax.fori_loop(1, planes, greet, 0)
    pl.semaphore_wait(barrier, 3 + planes - 1)

    def copy(it, slot, kind, d, target):
        return pltpu.make_async_remote_copy(
            src_ref=field.at[it, slot],
            dst_ref=field.at[it, slot],
            send_sem=send_sem.at[kind, d],
            recv_sem=recv_sem.at[it % 2, slot],
            device_id=(target,),
            device_id_type=MESH,
        )

    def column(d):
        return lax.rem(z + planes - d, planes) * PLANE + low

    def arrived(it, slot):
        copy(it, slot, 0, 0, me + dp).wait_recv()

    def spread(it, d):
        col = column(d)
        copy(it, col, 1, d, me + da).start()
        copy(it, col, 2, d, me + db).start()
        copy(it, col, 0, d, me + dp).start()

    def own_sends(it):
        def line(d, carry):
            copy(it, me, 7, d, lax.rem(z + d, planes) * PLANE + low).start()
            return carry

        spread(it, 0)
        lax.fori_loop(1, planes, line, 0)

    def from_line(it, d):
        arrived(it, column(d))
        spread(it, d)

    def across(it, d):
        col = column(d)
        arrived(it, col + db)
        copy(it, col + db, 3, d, me + da).start()
        copy(it, col + db, 4, d, me + dp).start()
        arrived(it, col + da)
        copy(it, col + da, 5, d, me + dp).start()

    def sends_done(it):
        def one(d, carry):
            for kind in range(7):
                copy(it, me, kind, d, me + dp).wait_send()
            return carry

        def line(d, carry):
            copy(it, me, 7, d, me + dp).wait_send()
            return carry

        lax.fori_loop(0, planes, one, 0)
        lax.fori_loop(1, planes, line, 0)

    tile = min(512, rows)

    def multiply(it, d):
        col = column(d)
        plane = col // PLANE
        arrived(it, col + da + db)
        copy(it, col + da + db, 6, d, me + dp).start()
        for delta in (0, da, db, da + db):
            arrived(it, col + dp + delta)
        for part in range(PLANE):
            v = field[it, plane * PLANE + part]
            hi = v.astype(jnp.bfloat16)
            lo = (v - hi.astype(jnp.float32)).astype(jnp.bfloat16)
            for half in range(2):
                at = half * kp + part * local
                wmat[at : at + local, :scen] = hi
                wmat[at : at + local, scen:] = lo

        @pl.loop(0, rows // tile)
        def _(m):
            at = pl.ds(pl.multiple_of(m * tile, tile), tile)
            out = jnp.dot(pmat[plane, at, :], wmat[...], preferred_element_type=jnp.float32)
            acc[at, :] += out[:, :scen] + out[:, scen:]

    group = min(16, local)

    def finish(it):
        @pl.loop(0, local // group)
        def _(g):
            at = pl.ds(pl.multiple_of(g * group * actions, group * actions), group * actions)
            q = acc[at, :].reshape(group, actions, scen)
            rel_ref[pl.ds(pl.multiple_of(g * group, group), group), :] = jnp.min(q, axis=1)

        best = rel_ref[...]

        if not isinstance(it, int) or it < ITERS - 1:
            @pl.when(it < ITERS - 1)
            def _():
                field[it + 1, me] = best

        increase = best - field[it, me]
        sbuf[0, pl.ds(it, 1), :] = jnp.max(increase, axis=0, keepdims=True)
        sbuf[0, pl.ds(ITERS + it, 1), :] = -jnp.min(increase, axis=0, keepdims=True)
        acc[...] = costs[...]

    sbuf[0] = jnp.full(sbuf.shape[1:], -big_value, jnp.float32)
    start_copy.wait()
    own_sends(0)

    def convert(c, carry):
        load(c).wait()
        slot = lax.rem(c, slots)

        @pl.loop(0, chunk // 16)
        def _(r):
            src = pl.ds(pl.multiple_of(r * 16, 16), 16)
            dst = pl.ds(pl.multiple_of(c * chunk + r * 16, 16), 16)
            for plane in range(planes):
                x = stage[slot, src, plane * kp : (plane + 1) * kp]
                hi = x.astype(jnp.bfloat16)
                pmat[plane, dst, :kp] = hi
                pmat[plane, dst, kp:] = (x - hi.astype(jnp.float32)).astype(jnp.bfloat16)

        @pl.when(c + slots < chunks)
        def _():
            load(c + slots).start()

        return carry

    def each(begin, end, step, it):
        def one(d, carry):
            step(it, d)
            return carry

        lax.fori_loop(begin, end, one, 0)

    lax.fori_loop(0, chunks // 2, convert, 0)
    each(1, planes, from_line, 0)
    across(0, 0)
    lax.fori_loop(chunks // 2, 3 * chunks // 4, convert, 0)
    each(1, planes, across, 0)
    lax.fori_loop(3 * chunks // 4, chunks, convert, 0)

    cost_copy.wait()

    @pl.loop(0, local)
    def _(s):
        at = pl.ds(pl.multiple_of(s * actions, actions), actions)
        allowed = lax.broadcasted_iota(jnp.int32, (actions, scen), 0) < vc_ref[s]
        masked = jnp.where(allowed, costs[at, :], jnp.float32(big_value))
        costs[at, :] = masked
        acc[at, :] = masked

    each(0, planes, multiply, 0)
    finish(0)
    sends_done(0)

    def iteration(it, carry):
        own_sends(it)

        def step(d, carry):
            @pl.when(jnp.logical_and(d >= 1, d < planes))
            def _():
                from_line(it, d)

            @pl.when(jnp.logical_and(d >= 1, d < planes + 1))
            def _():
                across(it, d - 1)

            @pl.when(d >= 2)
            def _():
                multiply(it, d - 2)

            return carry

        lax.fori_loop(1, planes + 2, step, 0)
        finish(it)
        sends_done(it)
        return carry

    lax.fori_loop(1, ITERS, iteration, 0)

    position = lax.broadcasted_iota(jnp.int32, (local, scen), 0) + me * local
    chosen = jnp.where(position == ref_ref[0], rel_ref[...], jnp.float32(-big_value))
    sbuf[0, 2 * ITERS : 2 * ITERS + 1, :] = jnp.max(chosen, axis=0, keepdims=True)

    def reduce_copy(source, slot, target):
        return pltpu.make_async_remote_copy(
            src_ref=sbuf.at[source],
            dst_ref=rbuf.at[slot],
            send_sem=rsend_sem.at[slot],
            recv_sem=rrecv_sem.at[slot],
            device_id=(target,),
            device_id_type=MESH,
        )

    for number, delta in enumerate((dp, da, db)):
        step = reduce_copy(number, number, me + delta)
        step.start()
        step.wait_recv()
        sbuf[number + 1] = jnp.maximum(sbuf[number], rbuf[number])
        step.wait_send()

    def along(d):
        return reduce_copy(3, 2 + d, lax.rem(z + d, planes) * PLANE + low)

    def send(d, carry):
        along(d).start()
        return carry

    def take(d, total):
        along(d).wait_recv()
        return jnp.maximum(total, rbuf[2 + d])

    def sent(d, carry):
        along(d).wait_send()
        return carry

    lax.fori_loop(1, planes, send, 0)
    total = lax.fori_loop(1, planes, take, sbuf[3])
    lax.fori_loop(1, planes, sent, 0)
    up_ref[...] = total[:ITERS]
    low_ref[...] = -total[ITERS : 2 * ITERS]
    rel_ref[...] = rel_ref[...] - total[2 * ITERS : 2 * ITERS + 1]


def solution(mesh):
    n = mesh.shape["state"]

    def local_step(transitions, costs, valid_counts, start_values, ref_state):
        local, actions, states = transitions.shape
        scen = start_values.shape[1]
        rows = local * actions
        planes = n // PLANE
        kp = states // planes
        chunk = min(64, rows // 4)
        slots = min(8, rows // chunk)
        f32, bf16 = jnp.float32, jnp.bfloat16
        vmem = pl.BlockSpec(memory_space=pltpu.VMEM)
        smem = pl.BlockSpec(memory_space=pltpu.SMEM)
        hbm = pl.BlockSpec(memory_space=pl.ANY)
        rel, low, up = pl.pallas_call(
            functools.partial(kernel, n),
            out_shape=(
                jax.ShapeDtypeStruct((local, scen), f32),
                jax.ShapeDtypeStruct((ITERS, scen), f32),
                jax.ShapeDtypeStruct((ITERS, scen), f32),
            ),
            in_specs=[smem, smem, hbm, hbm, hbm],
            out_specs=(vmem, vmem, vmem),
            scratch_shapes=[
                pltpu.VMEM((ITERS, n, local, scen), f32),
                pltpu.VMEM((planes, rows, 2 * kp), bf16),
                pltpu.VMEM((2 * kp, 2 * scen), bf16),
                pltpu.VMEM((rows, scen), f32),
                pltpu.VMEM((rows, scen), f32),
                pltpu.VMEM((slots, chunk, states), f32),
                pltpu.VMEM((4, 16, scen), f32),
                pltpu.VMEM((2 + planes, 16, scen), f32),
                pltpu.SemaphoreType.DMA((slots,)),
                pltpu.SemaphoreType.DMA((2,)),
                pltpu.SemaphoreType.DMA((8, planes)),
                pltpu.SemaphoreType.DMA((2, n)),
                pltpu.SemaphoreType.DMA((2 + planes,)),
                pltpu.SemaphoreType.DMA((2 + planes,)),
            ],
            compiler_params=pltpu.CompilerParams(
                collective_id=0, has_side_effects=True, vmem_limit_bytes=66 * 1000 * 1000
            ),
        )(
            valid_counts, ref_state, transitions.reshape(rows, states),
            costs.reshape(rows, scen), start_values,
        )
        return rel, low, up

    in_specs = (P("state", None, None), P("state", None, None), P("state"), P("state", None), P())
    out_specs = (P("state", None), P(), P())
    return jax.shard_map(local_step, mesh=mesh, in_specs=in_specs, out_specs=out_specs, check_vma=False)
```
